256 devices in a mesh: fsdp: 16 (over z, core), cols: 16 (over y, x).
Axes of the slice: x: 4, y: 4, z: 8, core: 2. Of those that a mesh axis runs over, the one named last changes fastest.
Arguments:
- weight_gate: bfloat16 [4096, 11008], P('fsdp', 'cols'), may hold values from -0.09375 to 0.09375
- low_gate: bfloat16 [4096, 64], P('fsdp'), may hold values from -0.09375 to 0.09375
- high_gate: bfloat16 [64, 11008], P(None, 'cols'), may hold values from -0.75 to 0.75
- weight_up: bfloat16 [4096, 11008], P('fsdp', 'cols'), may hold values from -0.09375 to 0.09375
- low_up: bfloat16 [4096, 64], P('fsdp'), may hold values from -0.09375 to 0.09375
- high_up: bfloat16 [64, 11008], P(None, 'cols'), may hold values from -0.75 to 0.75
- weight_down: bfloat16 [11008, 4096], P('cols', 'fsdp'), may hold values from -0.0546875 to 0.0546875
- low_down: bfloat16 [11008, 64], P('cols'), may hold values from -0.0546875 to 0.0546875
- high_down: bfloat16 [64, 4096], P(None, 'fsdp'), may hold values from -0.75 to 0.75
- norm_train: float32 [4096], P(('fsdp', 'cols')), may hold values from 0.25 to 1.75
- norm_step: float32 [4096], P(('fsdp', 'cols')), may hold values from -0.3 to 0.3
Outputs:
- serve_gate: bfloat16 [11008, 4096], P('cols')
- serve_up: bfloat16 [11008, 4096], P('cols')
- serve_down: bfloat16 [4096, 11008], P(None, 'cols')
- serve_norm: bfloat16 [4096], replicated
The draws below stay inside these ranges and needn't reach their ends.
All inputs are finite; a program needn't handle non-finite values.
Results may differ from the reference program's by a relative error of at most 0.001.
Values may be sent and summed in bfloat16 or wider, within the bound.
A program may use at most 128 MiB of HBM per device.

```python
import jax
import jax.numpy as jnp

D_MODEL = 4096
D_INNER = 11008
RANK = 64


def block_scale(key, extent, pieces, low, high):
    factor_of, own = 1.0, jax.random.fold_in(key, 6)
    for axis_at, shards_of in pieces:
        draws = jnp.exp(jax.random.uniform(jax.random.fold_in(own, axis_at), (shards_of,), jnp.float32, low / len(pieces), high / len(pieces)))
        factor_of = factor_of * jnp.repeat(draws, extent[axis_at] // shards_of).reshape([-1 if axis == axis_at else 1 for axis in range(len(extent))])
    return factor_of


def scatter_about(key, shape, width, limit, pieces=(), kind=jnp.bfloat16):
    array = jax.random.normal(key, shape, jnp.float32) * width
    if len(pieces) > 0:
        array = block_scale(key, shape, pieces, -0.22, 0.18) * array
    return jnp.clip(array, min=-limit, max=limit).astype(kind)


def setup_inputs(seed: int = 0) -> dict:
    key_of = jax.random.split(jax.random.key(seed), 12)
    weight_gate = scatter_about(key_of[0], (D_MODEL, D_INNER), D_MODEL ** -0.5, 0.09375, ((0, 16), (1, 16)))
    low_gate = scatter_about(key_of[1], (D_MODEL, RANK), D_MODEL ** -0.5, 0.09375, ((0, 16),))
    high_gate = scatter_about(key_of[2], (RANK, D_INNER), RANK ** -0.5, 0.75, ((1, 16),))
    weight_up = scatter_about(key_of[3], (D_MODEL, D_INNER), D_MODEL ** -0.5, 0.09375, ((0, 16), (1, 16)))
    low_up = scatter_about(key_of[4], (D_MODEL, RANK), D_MODEL ** -0.5, 0.09375, ((0, 16),))
    high_up = scatter_about(key_of[5], (RANK, D_INNER), RANK ** -0.5, 0.75, ((1, 16),))
    weight_down = scatter_about(key_of[6], (D_INNER, D_MODEL), D_INNER ** -0.5, 0.0546875, ((0, 16), (1, 16)))
    low_down = scatter_about(key_of[7], (D_INNER, RANK), D_INNER ** -0.5, 0.0546875, ((0, 16),))
    high_down = scatter_about(key_of[8], (RANK, D_MODEL), RANK ** -0.5, 0.75, ((1, 16),))
    norm_train = jnp.clip(1.0 + 0.15 * jax.random.normal(key_of[9], (D_MODEL,), jnp.float32), 0.25, 1.75)
    norm_step = jnp.clip(jax.random.uniform(key_of[10], (D_MODEL,), jnp.float32, -0.3, 0.3) * block_scale(key_of[10], (D_MODEL,), ((0, 256),), -0.4, 0.0), -0.3, 0.3)
    return dict(weight_gate=weight_gate, low_gate=low_gate, high_gate=high_gate, weight_up=weight_up, low_up=low_up, high_up=high_up, weight_down=weight_down, low_down=low_down, high_down=high_down, norm_train=norm_train, norm_step=norm_step)


mix_rate = 0.5


def reference(weight_gate, low_gate, high_gate, weight_up, low_up, high_up, weight_down, low_down, high_down, norm_train, norm_step):
    fresh_gate = weight_gate.astype(jnp.float32) + mix_rate * jnp.dot(low_gate, high_gate, preferred_element_type=jnp.float32)
    fresh_up = weight_up.astype(jnp.float32) + mix_rate * jnp.dot(low_up, high_up, preferred_element_type=jnp.float32)
    fresh_down = weight_down.astype(jnp.float32) + mix_rate * jnp.dot(low_down, high_down, preferred_element_type=jnp.float32)
    serve_gate = fresh_gate.T.astype(jnp.bfloat16)
    serve_up = fresh_up.T.astype(jnp.bfloat16)
    serve_down = fresh_down.T.astype(jnp.bfloat16)
    serve_norm = (norm_train + norm_step).astype(jnp.bfloat16)
    return serve_gate, serve_up, serve_down, serve_norm
```

```python
import jax
import jax.numpy as jnp
from jax import lax
from jax.experimental import pallas as pl
from jax.experimental.pallas import tpu as pltpu
from jax.sharding import PartitionSpec as P

mix_rate = 0.5
MESH = pl.DeviceIdType.MESH
DMA = pltpu.SemaphoreType.DMA


def kernel(nf, nc, cut, *refs):
    ins, outs, norm_out = refs[0:11], refs[11:14], refs[14]
    held, norm_all = refs[15:26], refs[26]
    (in_sem, ring_send, ring_recv, pair_send, pair_recv, n1_send, n1_recv, n2_send, n2_recv) = refs[27:]
    nz = nf // 2
    far, near = nz // 2, nz // 2 - 1
    rows, width = ins[0].shape
    f, c = lax.axis_index("fsdp"), lax.axis_index("cols")
    z, core = f // 2, f % 2
    partner = z * 2 + 1 - core

    def at(dz):
        return lax.rem(z + dz + nz, nz) * 2 + core

    barrier = pltpu.get_barrier_semaphore()
    for k in range(1, nf):
        pl.semaphore_signal(barrier, inc=1, device_id={"fsdp": lax.rem(f + k, nf)}, device_id_type=MESH)
    for k in range(1, nc):
        pl.semaphore_signal(barrier, inc=1, device_id={"cols": lax.rem(c + k, nc)}, device_id_type=MESH)

    loads = [pltpu.make_async_copy(ins[i], held[i], in_sem.at[i]) for i in range(11)]
    for load in loads:
        load.start()

    def columns(source):
        return pl.ds(pl.multiple_of(source * width, width), width)

    def merge(a):
        for i in range(3 * a, 3 * a + 3):
            loads[i].wait()
        w, left, right = held[3 * a], held[3 * a + 1], held[3 * a + 2]
        product = lax.dot_general(
            left[...], right[...], (((0,), (0,)), ((), ())), preferred_element_type=jnp.float32
        )
        fresh = w[...].astype(jnp.float32) + mix_rate * product
        outs[a][:, columns(f)] = fresh.astype(jnp.bfloat16)

    spans = [[(0, cut), (cut, rows - cut)] for _ in range(3)]

    def block(a, half, source):
        start, size = spans[a][half]
        return outs[a].at[pl.ds(start, size), columns(source)]

    def hops(way, half):
        return far if way == half else near

    order = [[(a, half) for half in (way, 1 - way) for a in range(3)] for way in (0, 1)]

    def ring(way, step, a, half):
        source = at(-(step - 1) if way == 0 else step - 1)
        piece = block(a, half, source)
        return pltpu.make_async_remote_copy(
            src_ref=piece,
            dst_ref=piece,
            send_sem=ring_send.at[way, a, half],
            recv_sem=ring_recv.at[way, step - 1, a, half],
            device_id={"fsdp": at(1 if way == 0 else -1)},
            device_id_type=MESH,
        )

    def arrival(way, step, a, half):
        source = at(-step if way == 0 else step)
        piece = block(a, half, source)
        return pltpu.make_async_remote_copy(
            src_ref=piece,
            dst_ref=piece,
            send_sem=ring_send.at[way, a, half],
            recv_sem=ring_recv.at[way, step - 1, a, half],
            device_id={"fsdp": at(1 if way == 0 else -1)},
            device_id_type=MESH,
        )

    def to_partner(ref, a):
        return pltpu.make_async_remote_copy(
            src_ref=ref,
            dst_ref=ref,
            send_sem=pair_send.at[a],
            recv_sem=pair_recv.at[a],
            device_id={"fsdp": partner},
            device_id_type=MESH,
        )

    def send_own(a):
        for half in (0, 1):
            for way in (0, 1):
                ring(way, 1, a, half if way == 0 else 1 - half).start()
        to_partner(outs[a].at[:, columns(f)], a).start()

    loads[9].wait()
    loads[10].wait()
    gain = (held[9][...] + held[10][...]).astype(jnp.bfloat16)
    short = gain.shape[1]
    lanes = short * nc
    place = lax.broadcasted_iota(jnp.int32, (short, lanes), 1) == (
        lax.broadcasted_iota(jnp.int32, (short, lanes), 0) + c * short
    )
    placed = jnp.dot(
        jnp.broadcast_to(gain, (16, short)),
        place.astype(jnp.bfloat16),
        preferred_element_type=jnp.float32,
    )
    norm_all[c, f] = placed[0:1]

    merge(0)
    merge(1)
    pl.semaphore_wait(barrier, nf + nc - 2)

    def n1(k):
        row = norm_all.at[c, f]
        return pltpu.make_async_remote_copy(
            src_ref=row,
            dst_ref=row,
            send_sem=n1_send,
            recv_sem=n1_recv,
            device_id={"fsdp": lax.rem(f + k, nf)},
            device_id_type=MESH,
        )

    def n2(k):
        part = norm_all.at[c]
        return pltpu.make_async_remote_copy(
            src_ref=part,
            dst_ref=part,
            send_sem=n2_send,
            recv_sem=n2_recv,
            device_id={"cols": lax.rem(c + k, nc)},
            device_id_type=MESH,
        )

    for k in range(1, nf):
        n1(k).start()
    send_own(0)
    merge(2)
    send_own(1)
    send_own(2)

    def take(step):
        for i in range(6):
            for way in (0, 1):
                a, half = order[way][i]
                if step <= hops(way, half):
                    arrival(way, step, a, half).wait_recv()
                    if step < hops(way, half):
                        ring(way, step + 1, a, half).start()
                    source = at(-step if way == 0 else step)
                    to_partner(block(a, half, source), a).start()

    def wait_bytes(ref, sem):
        pltpu.make_async_copy(ref, ref, sem).wait()

    for step in range(1, far + 1):
        take(step)
        if step == 1:
            wait_bytes(norm_all.at[0, pl.ds(0, nf - 1)], n1_recv)
            for k in range(1, nc):
                n2(k).start()

    if nc > 1:
        wait_bytes(norm_all.at[pl.ds(0, nc - 1)], n2_recv)
        wait_bytes(norm_all.at[pl.ds(0, nc - 1)], n2_send)
    wait_bytes(norm_all.at[0, pl.ds(0, nf - 1)], n1_send)
    total = norm_all[0]
    for k in range(1, nc):
        total = total + norm_all[k]
    norm_out[...] = total

    for way in (0, 1):
        for a in range(3):
            for half in (0, 1):
                start, size = spans[a][half]
                wait_bytes(
                    outs[a].at[pl.ds(start, size), pl.ds(0, hops(way, half) * width)],
                    ring_send.at[way, a, half],
                )
    for a in range(3):
        wait_bytes(outs[a].at[:, pl.ds(0, nz * width)], pair_send.at[a])
        wait_bytes(outs[a].at[:, pl.ds(0, nz * width)], pair_recv.at[a])


def solution(mesh):
    nf, nc = mesh.shape["fsdp"], mesh.shape["cols"]

    def per_device(
        weight_gate, low_gate, high_gate, weight_up, low_up, high_up,
        weight_down, low_down, high_down, norm_train, norm_step,
    ):
        rows, width = weight_down.shape
        rank = low_down.shape[1]
        short = norm_train.shape[0]
        cut = (rows // 2 + 15) // 16 * 16
        far = nf // 4
        big = jax.ShapeDtypeStruct((rows, width * nf), jnp.bfloat16)
        gate, up, down, norm = pl.pallas_call(
            lambda *refs: kernel(nf, nc, cut, *refs),
            out_shape=(big, big, big, jax.ShapeDtypeStruct((nf, 1, short * nc), jnp.float32)),
            in_specs=[pl.BlockSpec(memory_space=pltpu.HBM)] * 11,
            out_specs=(pl.BlockSpec(memory_space=pltpu.VMEM),) * 4,
            scratch_shapes=[
                pltpu.VMEM((rows, width), jnp.bfloat16),
                pltpu.VMEM((rank, rows), jnp.bfloat16),
                pltpu.VMEM((rank, width), jnp.bfloat16),
            ] * 3
            + [
                pltpu.VMEM((1, short), jnp.float32),
                pltpu.VMEM((1, short), jnp.float32),
                pltpu.VMEM((nc, nf, 1, short * nc), jnp.float32),
                DMA((11,)),
                DMA((2, 3, 2)),
                DMA((2, far, 3, 2)),
                DMA((3,)),
                DMA((3,)),
                DMA, DMA, DMA, DMA,
            ],
            compiler_params=pltpu.CompilerParams(
                collective_id=0, has_side_effects=True, vmem_limit_bytes=VMEM_LIMIT
            ),
        )(*[pltpu.with_memory_space_constraint(x, pltpu.HBM) for x in (
            weight_gate.T, high_gate, low_gate.T,
            weight_up.T, high_up, low_up.T,
            weight_down, low_down.T, high_down,
            norm_train.reshape(1, short), norm_step.reshape(1, short),
        )])
        return gate, up, down.T, norm.astype(jnp.bfloat16).reshape(-1)

    both = ("fsdp", "cols")
    return jax.shard_map(
        per_device,
        mesh=mesh,
        in_specs=(
            P("fsdp", "cols"), P("fsdp", None), P(None, "cols"),
            P("fsdp", "cols"), P("fsdp", None), P(None, "cols"),
            P("cols", "fsdp"), P("cols", None), P(None, "fsdp"),
            P(both), P(both),
        ),
        out_specs=(P("cols", None), P("cols", None), P(None, "cols"), P()),
        check_vma=False,
    )


VMEM_LIMIT = 24 * 1024 * 1024
```

```python
import jax
import jax.numpy as jnp
from jax import lax
from jax.experimental import pallas as pl
from jax.experimental.pallas import tpu as pltpu
from jax.sharding import PartitionSpec as P

mix_rate = 0.5
MESH = pl.DeviceIdType.MESH
DMA = pltpu.SemaphoreType.DMA
LANES = 128
VMEM_LIMIT = 24 * 1024 * 1024


def gather_kernel(nf, nx, ny, cut, *refs):
    ins, outs, norm_rows = refs[0:11], refs[11:14], refs[14]
    held, norm_plane = refs[15:26], refs[26]
    (
        in_sem, ring_send, ring_recv, pair_send, pair_recv,
        x_send, x_recv, y_send, y_recv, n_send, n_recv, np_send, np_recv,
    ) = refs[27:]
    nz = nf // 2
    far, near = nz // 2, nz // 2 - 1
    rows, width = ins[0].shape
    f, c = lax.axis_index("fsdp"), lax.axis_index("cols")
    z, core = f // 2, f % 2
    y, x = c // nx, c % nx
    partner = z * 2 + 1 - core

    def at_z(dz):
        return lax.rem(z + dz + nz, nz) * 2 + core

    def at_x(dx):
        return y * nx + lax.rem(x + dx + nx, nx)

    def at_y(dy):
        return lax.rem(y + dy + ny, ny) * nx + x

    near_by = [("fsdp", partner)]
    near_by += [("fsdp", at_z(d)) for d in ((1, -1) if nz > 2 else (1,) if nz > 1 else ())]
    near_by += [("cols", at_x(d)) for d in ((1, -1) if nx > 2 else (1,) if nx > 1 else ())]
    near_by += [("cols", at_y(d)) for d in ((1, -1) if ny > 2 else (1,) if ny > 1 else ())]
    barrier = pltpu.get_barrier_semaphore()
    for axis, index in near_by:
        pl.semaphore_signal(barrier, inc=1, device_id={axis: index}, device_id_type=MESH)

    loads = [pltpu.make_async_copy(ins[i], held[i], in_sem.at[i]) for i in range(11)]
    for load in loads:
        load.start()

    def send(ref, axis, index, send_sem, recv_sem):
        return pltpu.make_async_remote_copy(
            src_ref=ref,
            dst_ref=ref,
            send_sem=send_sem,
            recv_sem=recv_sem,
            device_id={axis: index},
            device_id_type=MESH,
        )

    def wait_bytes(ref, sem):
        pltpu.make_async_copy(ref, ref, sem).wait()

    def columns(source):
        return pl.ds(pl.multiple_of(source * width, width), width)

    spans = [(0, cut), (cut, rows - cut)]

    def merge(a):
        for i in range(3 * a, 3 * a + 3):
            loads[i].wait()
        w, left, right = held[3 * a], held[3 * a + 1], held[3 * a + 2]
        product = lax.dot_general(
            left[...], right[...], (((0,), (0,)), ((), ())), preferred_element_type=jnp.float32
        )
        fresh = w[...].astype(jnp.float32) + mix_rate * product
        outs[a][:, columns(f)] = fresh.astype(jnp.bfloat16)

    def block(a, half, source):
        start, size = spans[half]
        return outs[a].at[pl.ds(start, size), columns(source)]

    def hops(way, half):
        return far if way == half else near

    order = [[(a, half) for half in (way, 1 - way) for a in range(3)] for way in (0, 1)]
    ahead = (1, -1)

    def ring(way, step, a, half):
        return send(
            block(a, half, at_z(-ahead[way] * (step - 1))),
            "fsdp",
            at_z(ahead[way]),
            ring_send.at[way, a, half],
            ring_recv.at[way, step - 1, a, half],
        )

    def to_partner(ref, a):
        return send(ref, "fsdp", partner, pair_send.at[a], pair_recv.at[a])

    def norm_hops(way):
        return hops(way, 0)

    def norm_ring(way, step):
        return send(
            norm_rows.at[at_z(-ahead[way] * (step - 1))],
            "fsdp",
            at_z(ahead[way]),
            n_send.at[way, step - 1],
            n_recv.at[way, step - 1],
        )

    def norm_to_partner(source):
        return send(norm_rows.at[source], "fsdp", partner, np_send, np_recv)

    loads[9].wait()
    loads[10].wait()
    gain = (held[9][...] + held[10][...]).astype(jnp.bfloat16)
    short = gain.shape[1]
    tiles = norm_rows.shape[1]
    spread = lax.broadcasted_iota(jnp.int32, (short, LANES), 1)
    index = lax.broadcasted_iota(jnp.int32, (short, LANES), 0) + c * short
    for t in range(tiles):
        place = (spread + t * LANES == index).astype(jnp.bfloat16)
        placed = jnp.dot(
            jnp.broadcast_to(gain, (16, short)), place, preferred_element_type=jnp.float32
        )
        norm_plane[y, x, t : t + 1] = placed[0:1]

    merge(0)
    merge(1)
    pl.semaphore_wait(barrier, len(near_by))

    def send_own(i):
        for way in (0, 1):
            a, half = order[way][i]
            ring(way, 1, a, half).start()

    def x_hop(way, step):
        source = lax.rem(x - ahead[way] * (step - 1) + nx, nx)
        return send(
            norm_plane.at[y, source], "cols", at_x(ahead[way]),
            x_send.at[way, step - 1], x_recv.at[way, step - 1],
        )

    def y_hop(way, step):
        source = lax.rem(y - ahead[way] * (step - 1) + ny, ny)
        return send(
            norm_plane.at[source], "cols", at_y(ahead[way]),
            y_send.at[way, step - 1], y_recv.at[way, step - 1],
        )

    def around(hop, n):
        counts = (n // 2, n - 1 - n // 2)
        for way in (0, 1):
            if counts[way] > 0:
                hop(way, 1).start()
        yield
        for step in range(1, max(counts) + 1):
            for way in (0, 1):
                if step <= counts[way]:
                    hop(way, step).wait_recv()
                    if step < counts[way]:
                        hop(way, step + 1).start()
        for way in (0, 1):
            for step in range(1, counts[way] + 1):
                hop(way, step).wait_send()

    xs, ys = around(x_hop, nx), around(y_hop, ny)
    next(xs)
    send_own(0)
    send_own(1)
    merge(2)
    send_own(2)
    for _ in xs:
        pass
    next(ys)
    to_partner(outs[0].at[:, columns(f)], 0).start()
    to_partner(outs[1].at[:, columns(f)], 1).start()
    for _ in ys:
        pass
    total = jnp.zeros((tiles, LANES), jnp.float32)
    for j in range(ny):
        for i in range(nx):
            total = total + norm_plane[j, i]
    norm_rows[f] = total
    to_partner(outs[2].at[:, columns(f)], 2).start()
    send_own(3)
    for way in (0, 1):
        if norm_hops(way) > 0:
            norm_ring(way, 1).start()
    norm_to_partner(f).start()
    send_own(4)
    send_own(5)

    for step in range(1, far + 1):
        for i in range(6):
            for way in (0, 1):
                a, half = order[way][i]
                if step <= hops(way, half):
                    ring(way, step, a, half).wait_recv()
                    if step < hops(way, half):
                        ring(way, step + 1, a, half).start()
                    to_partner(block(a, half, at_z(-ahead[way] * step)), a).start()
            if i == 2:
                for way in (0, 1):
                    if step <= norm_hops(way):
                        norm_ring(way, step).wait_recv()
                        if step < norm_hops(way):
                            norm_ring(way, step + 1).start()
                        norm_to_partner(at_z(-ahead[way] * step)).start()

    for way in (0, 1):
        for step in range(1, norm_hops(way) + 1):
            norm_ring(way, step).wait_send()
        for a in range(3):
            for half in (0, 1):
                start, size = spans[half]
                if hops(way, half) > 0:
                    wait_bytes(
                        outs[a].at[pl.ds(start, size), pl.ds(0, hops(way, half) * width)],
                        ring_send.at[way, a, half],
                    )
    wait_bytes(norm_rows.at[pl.ds(0, nz)], np_send)
    wait_bytes(norm_rows.at[pl.ds(0, nz)], np_recv)
    for a in range(3):
        wait_bytes(outs[a].at[:, pl.ds(0, nz * width)], pair_send.at[a])
        wait_bytes(outs[a].at[:, pl.ds(0, nz * width)], pair_recv.at[a])


def store_kernel(parts, *refs):
    ins, norm_rows, outs, norm_out = refs[0:3], refs[3], refs[4:7], refs[7]
    wide, narrow, sems, norm_sem = refs[8:]
    rows = ins[0].shape[0]
    size = -(-rows // (16 * parts)) * 16
    copies = []
    for a in range(3):
        for k in range(-(-rows // size)):
            span = pl.ds(k * size, min(size, rows - k * size))
            copies.append(
                pltpu.make_async_copy(ins[a].at[span], outs[a].at[span], sems.at[a, k])
            )
    for copy in copies:
        copy.start()
    count, tiles = norm_rows.shape[0:2]
    for i in range(count):
        wide[i * tiles : (i + 1) * tiles] = norm_rows[i]
    narrow[...] = wide[...].astype(jnp.bfloat16)
    last = pltpu.make_async_copy(narrow, norm_out, norm_sem)
    last.start()
    for copy in copies:
        copy.wait()
    last.wait()


def solution(mesh):
    nf, nc = mesh.shape["fsdp"], mesh.shape["cols"]
    nx = 4 if nc == 16 else 2 if nc == 4 else nc
    ny = nc // nx
    vmem, hbm = pl.BlockSpec(memory_space=pltpu.VMEM), pl.BlockSpec(memory_space=pltpu.HBM)

    def per_device(
        weight_gate, low_gate, high_gate, weight_up, low_up, high_up,
        weight_down, low_down, high_down, norm_train, norm_step,
    ):
        rows, width = weight_down.shape
        rank = low_down.shape[1]
        short = norm_train.shape[0]
        tiles = short * nc // LANES
        cut = (rows // 2 + 15) // 16 * 16
        far = nf // 4
        big = jax.ShapeDtypeStruct((rows, width * nf), jnp.bfloat16)
        whole = pl.pallas_call(
            lambda *refs: gather_kernel(nf, nx, ny, cut, *refs),
            out_shape=(big, big, big, jax.ShapeDtypeStruct((nf, tiles, LANES), jnp.float32)),
            in_specs=[hbm] * 11,
            out_specs=(vmem,) * 4,
            scratch_shapes=[
                pltpu.VMEM((rows, width), jnp.bfloat16),
                pltpu.VMEM((rank, rows), jnp.bfloat16),
                pltpu.VMEM((rank, width), jnp.bfloat16),
            ] * 3
            + [
                pltpu.VMEM((1, short), jnp.float32),
                pltpu.VMEM((1, short), jnp.float32),
                pltpu.VMEM((ny, nx, tiles, LANES), jnp.float32),
                DMA((11,)),
                DMA((2, 3, 2)),
                DMA((2, far, 3, 2)),
                DMA((3,)),
                DMA((3,)),
                DMA((2, 2)), DMA((2, 2)), DMA((2, 2)), DMA((2, 2)),
                DMA((2, far)), DMA((2, far)), DMA, DMA,
            ],
            compiler_params=pltpu.CompilerParams(
                collective_id=0, has_side_effects=True, vmem_limit_bytes=VMEM_LIMIT
            ),
        )(*[pltpu.with_memory_space_constraint(operand, pltpu.HBM) for operand in (
            weight_gate.T, high_gate, low_gate.T,
            weight_up.T, high_up, low_up.T,
            weight_down, low_down.T, high_down,
            norm_train.reshape(1, short), norm_step.reshape(1, short),
        )])
        parts = 4
        gate, up, down, norm = pl.pallas_call(
            lambda *refs: store_kernel(parts, *refs),
            out_shape=(big, big, big, jax.ShapeDtypeStruct((nf * tiles, LANES), jnp.bfloat16)),
            in_specs=[vmem] * 4,
            out_specs=(hbm,) * 4,
            scratch_shapes=[
                pltpu.VMEM((nf * tiles, LANES), jnp.float32),
                pltpu.VMEM((nf * tiles, LANES), jnp.bfloat16),
                DMA((3, parts)),
                DMA,
            ],
            compiler_params=pltpu.CompilerParams(vmem_limit_bytes=VMEM_LIMIT),
        )(*whole)
        return gate, up, down.T, norm.reshape(-1)

    both = ("fsdp", "cols")
    return jax.shard_map(
        per_device,
        mesh=mesh,
        in_specs=(
            P("fsdp", "cols"), P("fsdp", None), P(None, "cols"),
            P("fsdp", "cols"), P("fsdp", None), P(None, "cols"),
            P("cols", "fsdp"), P("cols", None), P(None, "fsdp"),
            P(both), P(both),
        ),
        out_specs=(P("cols", None), P("cols", None), P(None, "cols"), P()),
        check_vma=False,
    )
```
